32 devices in a mesh: section: 4 (over z), ctx: 4 (over x, core), tp: 2 (over y).
Axes of the slice: x: 2, y: 2, z: 4, core: 2. Of those that a mesh axis runs over, the one named last changes fastest.
Arguments:
- queries: bfloat16 [4, 512, 8192], P('section', 'ctx', 'tp'), may hold values from -80 to 80
- keys: bfloat16 [4, 512, 1024], P('section', 'ctx', 'tp'), may hold values from -4 to 4
- values: bfloat16 [4, 512, 1024], P('section', 'ctx', 'tp'), may hold values from -6 to 6
- span_order: int32 [8], replicated, may hold values from 0 to 7, as said below
Outputs:
- attended: bfloat16 [4, 512, 8192], P('section', ('ctx', 'tp'))
The draws below stay inside these ranges and needn't reach their ends.
Inputs may be any that keep to these rules, and one draw needn't show every extreme that they name: `span_order`: a permutation of 0 to 7 in which entries 2 c and 2 c + 1 sum to 7 for every c.
All inputs are finite; a program needn't handle non-finite values.
Results may differ from the reference program's by a relative error of at most 0.0055.
Values may be sent and summed in bfloat16 or wider, within the bound.
A program may use at most 64 MiB of HBM per device.

```python
import jax
import jax.numpy as jnp
from jax import lax

QUERY_HEADS = 64
KEY_VALUE_HEADS = 8
HEAD_DIMENSION = 128
TOK_DEV = 128
SEQUENCE_TOKENS = 512
N_SECTION = 4
N_CTX = 4


def paired_order(key):
    folded = jax.random.fold_in(key, 11)
    shuffled = jax.random.permutation(folded, N_CTX).astype(jnp.int32)
    flipped = jax.random.randint(jax.random.fold_in(folded, 1), (N_CTX,), 0, 2).astype(jnp.int32)
    lower_half = shuffled
    upper_half = 2 * N_CTX - 1 - shuffled
    first_entry = jnp.where(flipped == 1, upper_half, lower_half)
    second_entry = jnp.where(flipped == 1, lower_half, upper_half)
    return jnp.stack([first_entry, second_entry], axis=1).reshape(2 * N_CTX).astype(jnp.int32)


def key_rows(key):
    unpermuted = jax.random.truncated_normal(jax.random.fold_in(key, 21), -4.0, 4.0, (N_SECTION, SEQUENCE_TOKENS, KEY_VALUE_HEADS * HEAD_DIMENSION), jnp.float32)
    return unpermuted


def draw_span_order(key, part):
    return paired_order(key)


def draw_keys(key, part):
    unpermuted = key_rows(key)
    return unpermuted.astype(jnp.bfloat16)


def draw_queries(key, part):
    result = jax.random.truncated_normal(jax.random.fold_in(key, 31), -4.0, 4.0, (N_SECTION, SEQUENCE_TOKENS, QUERY_HEADS * HEAD_DIMENSION), jnp.float32)
    return result.astype(jnp.bfloat16)


def level_of(rng, shape, cuts, low, largest):
    loudness, own = 1.0, jax.random.fold_in(rng, 6)
    for dim, shards_of in cuts:
        steps = jnp.exp(jax.random.uniform(jax.random.fold_in(own, dim), (shards_of,), jnp.float32, low / len(cuts), largest / len(cuts)))
        loudness = loudness * jnp.repeat(steps, shape[dim] // shards_of).reshape([-1 if axis == dim else 1 for axis in range(len(shape))])
    return loudness


def scatter_about(rng, dims, scale, limit, pieces=(), held_as=jnp.bfloat16):
    drawn = jax.random.normal(rng, dims, jnp.float32) * scale
    if len(pieces) > 0:
        drawn = level_of(rng, dims, pieces, -0.22, 0.18) * drawn
    return jnp.clip(drawn, min=-limit, max=limit).astype(held_as)


def setup_inputs(seed: int = 0) -> dict:
    streams_of = jax.random.split(jax.random.key(seed), 5)
    queries = draw_queries(jax.random.fold_in(streams_of[4], 71), 0)
    keys = draw_keys(jax.random.fold_in(streams_of[4], 71), 0)
    values = scatter_about(streams_of[2], (N_SECTION, SEQUENCE_TOKENS, KEY_VALUE_HEADS * HEAD_DIMENSION), 1.0, 6.0, ((0, 4), (1, 4), (2, 2)))
    span_order = draw_span_order(jax.random.fold_in(streams_of[4], 71), 0)
    return {"queries": queries, "keys": keys, "values": values, "span_order": span_order}


def token_positions(order):
    row_index = jnp.arange(SEQUENCE_TOKENS, dtype=jnp.int32)
    span_rows = TOK_DEV // 2
    return (order[row_index // span_rows] * span_rows + row_index % span_rows).astype(jnp.int32)

def reference(queries, keys, values, span_order):
    group_size = QUERY_HEADS // KEY_VALUE_HEADS
    received_queries = jnp.roll(queries, 1, axis=0)
    received_keys = jnp.roll(keys, 1, axis=0)
    received_values = jnp.roll(values, 1, axis=0)
    where_pos = token_positions(span_order)
    query_head_rows = received_queries.astype(jnp.float32).reshape(N_SECTION, SEQUENCE_TOKENS, KEY_VALUE_HEADS, group_size, HEAD_DIMENSION)
    query_head_rows = query_head_rows.transpose(0, 2, 1, 3, 4).reshape(N_SECTION * KEY_VALUE_HEADS, SEQUENCE_TOKENS, group_size, HEAD_DIMENSION)
    key_head_rows = received_keys.astype(jnp.float32).reshape(N_SECTION, SEQUENCE_TOKENS, KEY_VALUE_HEADS, HEAD_DIMENSION)
    key_head_rows = key_head_rows.transpose(0, 2, 1, 3).reshape(N_SECTION * KEY_VALUE_HEADS, SEQUENCE_TOKENS, HEAD_DIMENSION)
    value_head_rows = received_values.astype(jnp.float32).reshape(N_SECTION, SEQUENCE_TOKENS, KEY_VALUE_HEADS, HEAD_DIMENSION)
    value_head_rows = value_head_rows.transpose(0, 2, 1, 3).reshape(N_SECTION * KEY_VALUE_HEADS, SEQUENCE_TOKENS, HEAD_DIMENSION)
    score_scale = 1.0 / jnp.sqrt(jnp.float32(HEAD_DIMENSION))
    starts = jnp.arange(SEQUENCE_TOKENS // TOK_DEV, dtype=jnp.int32) * TOK_DEV

    def one_head(operands):
        head_q, head_k, head_v = operands

        def one_block(first_row):
            block_q = lax.dynamic_slice_in_dim(head_q, first_row, TOK_DEV, 0)
            block_pos = lax.dynamic_slice_in_dim(where_pos, first_row, TOK_DEV, 0)
            scores = jnp.einsum('qgd,sd->gqs', block_q, head_k, precision=lax.Precision.HIGHEST) * score_scale
            allowed = where_pos[None, :] <= block_pos[:, None]
            row_max = lax.optimization_barrier(jnp.max(jnp.where(allowed[None], scores, jnp.float32(-1e+30)), axis=-1))
            weights = jnp.where(allowed[None], jnp.exp(scores - row_max[..., None]), jnp.float32(0.0))
            denominator = lax.optimization_barrier(jnp.sum(weights, axis=-1))
            rounded = lax.optimization_barrier(weights.astype(jnp.bfloat16)).astype(jnp.float32)
            summed = jnp.einsum('gqs,sd->gqd', rounded, head_v, precision=lax.Precision.HIGHEST)
            result = summed / denominator[..., None]
            return result.transpose(1, 0, 2).astype(jnp.bfloat16)
        return lax.map(one_block, starts)
    block_list = lax.map(one_head, (query_head_rows, key_head_rows, value_head_rows))
    block_list = block_list.reshape(N_SECTION, KEY_VALUE_HEADS, SEQUENCE_TOKENS, group_size, HEAD_DIMENSION).transpose(0, 2, 1, 3, 4)
    return block_list.reshape(N_SECTION, SEQUENCE_TOKENS, QUERY_HEADS * HEAD_DIMENSION)
```

```python
import functools
import math

import jax
import jax.numpy as jnp
from jax import lax
from jax.experimental import pallas as pl
from jax.experimental.pallas import tpu as pltpu
from jax.sharding import PartitionSpec as P

HEAD = 128
MESH = pl.DeviceIdType.MESH
NEG = -1e30


def lanes(start, size):
    return pl.ds(pl.multiple_of(start, HEAD), size)


def kernel(
    n_sec, n_ctx, n_tp, heads_per_chunk,
    q_hbm, k_hbm, v_hbm, order_hbm, out_hbm,
    q_buf, q_in, k_own, v_own, k_all, v_all, o_buf, bias, order,
    q_sem, own_sem, order_sem, kv_send, kv_recv, z_send, z_recv, o_send, o_recv,
):
    sec, ctx, tp = lax.axis_index("section"), lax.axis_index("ctx"), lax.axis_index("tp")
    rows, q_cols = q_hbm.shape[1], q_hbm.shape[2]
    kv_heads = k_hbm.shape[2] // HEAD
    group = q_cols // k_hbm.shape[2]
    g = heads_per_chunk
    chunk_cols = g * HEAD
    chunks = q_cols // chunk_cols
    per_kv = group // g
    out_rows = rows // n_tp
    keys = rows * n_ctx
    span = rows // 2
    local = kv_heads - 1
    group_cols = group * HEAD
    moved_cols = pl.ds(local * group_cols, group_cols)
    nxt, prv = lax.rem(sec + 1, n_sec), lax.rem(sec + n_sec - 1, n_sec)

    barrier = pltpu.get_barrier_semaphore()
    for t in range(n_tp):
        pl.semaphore_signal(barrier, inc=1, device_id=(prv, ctx, t), device_id_type=MESH)
    for d in range(1, n_ctx):
        pl.semaphore_signal(
            barrier, inc=1, device_id=(sec, lax.rem(ctx + d, n_ctx), tp), device_id_type=MESH
        )
    for d in range(1, n_tp):
        pl.semaphore_signal(
            barrier, inc=1, device_id=(sec, ctx, lax.rem(tp + d, n_tp)), device_id_type=MESH
        )
    own = []
    for i, (src, dst) in enumerate(((k_hbm, k_own), (v_hbm, v_own))):
        copy = pltpu.make_async_copy(src.at[0], dst, own_sem.at[i])
        copy.start()
        own.append(copy)
    order_copy = pltpu.make_async_copy(order_hbm, order, order_sem)
    order_copy.start()
    q_copies = []
    for i, h in enumerate([local, *range(local)]):
        cols = pl.ds(h * group_cols, group_cols)
        copy = pltpu.make_async_copy(q_hbm.at[0, :, cols], q_buf.at[:, cols], q_sem.at[i])
        copy.start()
        q_copies.append(copy)

    own[0].wait()
    own[1].wait()
    pl.semaphore_wait(barrier, n_ctx - 1 + n_tp + n_tp - 1)
    mine = pl.ds(pl.multiple_of(ctx * rows, rows), rows)

    def kv_copy(i, h, d):
        src, dst = ((k_own, k_all), (v_own, v_all))[i]
        peer = lax.rem(ctx + d, n_ctx)
        return pltpu.make_async_remote_copy(
            src_ref=src.at[:, pl.ds(h * HEAD, HEAD)] if h < local else dst.at[h, mine, :],
            dst_ref=dst.at[h, mine, :],
            send_sem=kv_send.at[h, i, d],
            recv_sem=kv_recv.at[h, i, d],
            device_id=(sec, peer, tp),
            device_id_type=MESH,
        )

    def kv_arrived(i, h, d):
        dst = (k_all, v_all)[i]
        peer = lax.rem(ctx + n_ctx - d, n_ctx)
        here = dst.at[h, pl.ds(pl.multiple_of(peer * rows, rows), rows), :]
        return pltpu.make_async_remote_copy(
            src_ref=here,
            dst_ref=here,
            send_sem=kv_send.at[h, i, d],
            recv_sem=kv_recv.at[h, i, d],
            device_id=(sec, lax.rem(ctx + d, n_ctx), tp),
            device_id_type=MESH,
        )

    def section_copy(i):
        if i < 2:
            src, dst = ((k_own, k_all), (v_own, v_all))[i]
            src, dst = src.at[:, pl.ds(local * HEAD, HEAD)], dst.at[local, mine, :]
        else:
            src, dst = q_buf.at[:, moved_cols], q_in
        return pltpu.make_async_remote_copy(
            src_ref=src,
            dst_ref=dst,
            send_sem=z_send.at[i],
            recv_sem=z_recv.at[i],
            device_id=(nxt, ctx, tp),
            device_id_type=MESH,
        )

    for h in range(local):
        for i in range(2):
            for d in range(1, n_ctx):
                kv_copy(i, h, d).start()
        if h == 0:
            section_copy(0).start()
            section_copy(1).start()
            q_copies[0].wait()
            section_copy(2).start()
    for h in range(local):
        k_all[h, mine, :] = k_own[:, h * HEAD : (h + 1) * HEAD]
        v_all[h, mine, :] = v_own[:, h * HEAD : (h + 1) * HEAD]

    order_copy.wait()
    row = lax.broadcasted_iota(jnp.int32, (rows, 1), 0)
    row_pos = jnp.where(row < span, order[2 * ctx] * span, order[2 * ctx + 1] * span - span) + row
    lane = lax.broadcasted_iota(jnp.int32, (1, keys), 1)
    key_pos = lane
    for j in range(keys // span):
        key_pos = jnp.where(
            (lane >= j * span) & (lane < (j + 1) * span), lane + (order[j] - j) * span, key_pos
        )
    bias[...] = jnp.where(key_pos <= row_pos, jnp.float32(0.0), jnp.float32(NEG))

    scale = math.log2(math.e) / math.sqrt(HEAD)

    def out_copy(c, t):
        return pltpu.make_async_remote_copy(
            src_ref=o_buf.at[c, pl.ds(pl.multiple_of(t * out_rows, out_rows), out_rows), :],
            dst_ref=out_hbm.at[0, :, lanes(tp * q_cols + c * chunk_cols, chunk_cols)],
            send_sem=o_send.at[c, t],
            recv_sem=o_recv.at[c, tp],
            device_id=(nxt, ctx, t),
            device_id_type=MESH,
        )

    def moved_out(c, d):
        t = lax.rem(tp + d, n_tp)
        src = o_buf.at[c, pl.ds(pl.multiple_of(t * out_rows, out_rows), out_rows), :]
        dst = out_hbm.at[0, :, lanes(tp * q_cols + c * chunk_cols, chunk_cols)]
        if d == 0:
            return pltpu.make_async_copy(src, dst, o_send.at[c, 0])
        return pltpu.make_async_remote_copy(
            src_ref=src,
            dst_ref=dst,
            send_sem=o_send.at[c, d],
            recv_sem=o_recv.at[c, tp],
            device_id=(sec, ctx, t),
            device_id_type=MESH,
        )

    for h in range(kv_heads):
        if h < local:
            q_copies[h + 1].wait()
        for d in range(1, n_ctx):
            kv_arrived(0, h, d).wait_recv()
        for d in range(1, n_ctx):
            kv_arrived(1, h, d).wait_recv()

        def chunk(i, _, h=h):
            c = h * per_kv + i
            q_ref, first = (q_buf, c * g) if h < local else (q_in, i * g)
            q = jnp.concatenate(
                [q_ref[:, lanes((first + j) * HEAD, HEAD)] for j in range(g)], axis=0
            )
            s = lax.dot_general(
                q, k_all[h], (((1,), (1,)), ((), ())), preferred_element_type=jnp.float32
            )
            s = s.reshape(g, rows, keys) * scale + bias[...][None]
            m = jnp.max(s, axis=-1, keepdims=True)
            p = jnp.exp2(s - m)
            total = jnp.sum(p, axis=-1, keepdims=True)
            o = jnp.dot(
                p.astype(jnp.bfloat16).reshape(g * rows, keys),
                v_all[h],
                preferred_element_type=jnp.float32,
            ).reshape(g, rows, HEAD)
            o = (o / total).astype(jnp.bfloat16)
            for j in range(g):
                o_buf[c, :, j * HEAD : (j + 1) * HEAD] = o[j]
            if h < local:
                out_copy(c, 0).start()

                @pl.when(c > 0)
                def _():
                    for t in range(1, n_tp):
                        out_copy(c - 1, t).start()
            else:
                for d in range(n_tp):
                    moved_out(c, d).start()
            return 0

        lax.fori_loop(0, per_kv, chunk, 0)
        if h == local - 1:
            for t in range(1, n_tp):
                out_copy(local * per_kv - 1, t).start()
        if h == 0:
            for i in range(2):
                section_copy(i).wait_recv()
                for d in range(1, n_ctx):
                    kv_copy(i, local, d).start()
        if h == local - 1:
            section_copy(2).wait_recv()

    for i in range(3):
        section_copy(i).wait_send()
    for h in range(kv_heads):
        for i in range(2):
            for d in range(1, n_ctx):
                kv_copy(i, h, d).wait_send()

    def finish(c, _):
        for t in range(n_tp):
            out_copy(c, t).wait_send()
        for t in range(n_tp):
            there = out_hbm.at[0, :, lanes(t * q_cols + c * chunk_cols, chunk_cols)]
            pltpu.make_async_remote_copy(
                src_ref=there,
                dst_ref=there,
                send_sem=o_send.at[c, t],
                recv_sem=o_recv.at[c, t],
                device_id=(nxt, ctx, t),
                device_id_type=MESH,
            ).wait_recv()
        return 0

    def finish_moved(c, _):
        moved_out(c, 0).wait()
        for d in range(1, n_tp):
            moved_out(c, d).wait_send()
        for d in range(1, n_tp):
            t = lax.rem(tp + d, n_tp)
            there = out_hbm.at[0, :, lanes(t * q_cols + c * chunk_cols, chunk_cols)]
            pltpu.make_async_remote_copy(
                src_ref=there,
                dst_ref=there,
                send_sem=o_send.at[c, d],
                recv_sem=o_recv.at[c, t],
                device_id=(sec, ctx, t),
                device_id_type=MESH,
            ).wait_recv()
        return 0

    lax.fori_loop(local * per_kv, chunks, finish_moved, 0)
    lax.fori_loop(0, local * per_kv, finish, 0)


def shards(n_sec, n_ctx, n_tp, queries, keys, values, span_order):
    rows, q_cols, kv_cols = queries.shape[1], queries.shape[2], keys.shape[2]
    kv_heads = kv_cols // HEAD
    group = q_cols // kv_cols
    g = math.gcd(group, 4)
    chunks = q_cols // (g * HEAD)
    all_rows = rows * n_ctx
    dma = pltpu.SemaphoreType.DMA
    any_spec = pl.BlockSpec(memory_space=pl.ANY)
    return pl.pallas_call(
        functools.partial(kernel, n_sec, n_ctx, n_tp, g),
        out_shape=pltpu.VMEM((1, rows // n_tp, q_cols * n_tp), jnp.bfloat16),
        in_specs=[any_spec] * 4,
        out_specs=any_spec,
        scratch_shapes=[
            pltpu.VMEM((rows, q_cols), jnp.bfloat16),
            pltpu.VMEM((rows, group * HEAD), jnp.bfloat16),
            pltpu.VMEM((rows, kv_cols), jnp.bfloat16),
            pltpu.VMEM((rows, kv_cols), jnp.bfloat16),
            pltpu.VMEM((kv_heads, all_rows, HEAD), jnp.bfloat16),
            pltpu.VMEM((kv_heads, all_rows, HEAD), jnp.bfloat16),
            pltpu.VMEM((chunks, rows, g * HEAD), jnp.bfloat16),
            pltpu.VMEM((rows, all_rows), jnp.float32),
            pltpu.SMEM(span_order.shape, jnp.int32),
            dma((kv_heads,)),
            dma((2,)),
            dma,
            dma((kv_heads, 2, n_ctx)),
            dma((kv_heads, 2, n_ctx)),
            dma((3,)),
            dma((3,)),
            dma((chunks, n_tp)),
            dma((chunks, n_tp)),
        ],
        compiler_params=pltpu.CompilerParams(collective_id=0, has_side_effects=True),
    )(queries, keys, values, span_order)


def solution(mesh):
    sizes = [mesh.shape[axis] for axis in ("section", "ctx", "tp")]
    placed = P("section", "ctx", "tp")
    return jax.shard_map(
        functools.partial(shards, *sizes),
        mesh=mesh,
        in_specs=(placed, placed, placed, P()),
        out_specs=P("section", ("ctx", "tp"), None),
        check_vma=False,
    )
```

```python
import functools
import math

import jax
import jax.numpy as jnp
from jax import lax
from jax.experimental import pallas as pl
from jax.experimental.pallas import tpu as pltpu
from jax.sharding import PartitionSpec as P

HEAD = 128
MESH = pl.DeviceIdType.MESH
NEG = -1e30
EARLY = 1


def lanes(start, size):
    return pl.ds(pl.multiple_of(start, HEAD), size)


def kernel(
    n_sec, n_ctx, n_tp, heads_per_chunk,
    q_hbm, k_hbm, v_hbm, order_hbm, out_hbm,
    q_buf, q_in, kv_own, kv_all, o_buf, bias, order,
    q_sem, own_sem, order_sem, kv_send, kv_recv, z_send, z_recv,
    o_send, o_recv, m_send, m_recv, m_own, ctx_in, tp_in, next_in,
):
    sec, ctx, tp = lax.axis_index("section"), lax.axis_index("ctx"), lax.axis_index("tp")
    rows, q_cols = q_hbm.shape[1], q_hbm.shape[2]
    kv_heads = k_hbm.shape[2] // HEAD
    group = q_cols // k_hbm.shape[2]
    g = heads_per_chunk
    chunk_cols = g * HEAD
    chunks = q_cols // chunk_cols
    per_kv = group // g
    out_rows = rows // n_tp
    keys = rows * n_ctx
    span = rows // 2
    local = kv_heads - 1
    group_cols = group * HEAD
    moved_cols = pl.ds(local * group_cols, group_cols)
    nxt, prv = lax.rem(sec + 1, n_sec), lax.rem(sec + n_sec - 1, n_sec)

    def there(s, c, t):
        return dict(device_id=(s, c, t), device_id_type=MESH)

    early = lax.rem(ctx, 2) == EARLY
    partner = ctx + 1 - 2 * lax.rem(ctx, 2)
    barrier = pltpu.get_barrier_semaphore()
    pl.semaphore_signal(barrier, inc=1, **there(prv, ctx, tp))
    for d in range(1, n_ctx):
        peer = lax.rem(ctx + d, n_ctx)

        @pl.when(lax.rem(peer, 2) != EARLY)
        def _():
            pl.semaphore_signal(barrier, inc=1, **there(sec, peer, tp))

    @pl.when(jnp.logical_not(early))
    def _():
        for d in range(1, n_tp):
            pl.semaphore_signal(barrier, inc=1, **there(sec, ctx, lax.rem(tp + d, n_tp)))

    def arrived(ref, sem):
        pltpu.make_async_copy(ref, ref, sem).wait()

    def left(ref, sem):
        pltpu.make_async_remote_copy(
            src_ref=ref, dst_ref=ref, send_sem=sem, recv_sem=sem, **there(nxt, ctx, tp)
        ).wait_send()

    for i, src in enumerate((k_hbm, v_hbm)):
        pltpu.make_async_copy(src.at[0], kv_own.at[i], own_sem).start()
    order_copy = pltpu.make_async_copy(order_hbm, order, order_sem)
    order_copy.start()
    for i, cols in enumerate((moved_cols, pl.ds(0, local * group_cols))):
        pltpu.make_async_copy(q_hbm.at[0, :, cols], q_buf.at[:, cols], q_sem.at[i]).start()

    arrived(kv_own, own_sem)

    def greet_tp():
        for d in range(1, n_tp):
            pl.semaphore_signal(next_in, inc=1, **there(sec, ctx, lax.rem(tp + d, n_tp)))

    pl.semaphore_wait(barrier, jnp.where(early, 1, n_ctx + n_tp - 1))

    @pl.when(jnp.logical_not(early))
    def _():
        pl.semaphore_signal(ctx_in, inc=1, **there(sec, partner, tp))
        greet_tp()

    others = pl.ds(0, keys - rows)
    mine = pl.ds(pl.multiple_of(ctx * rows, rows), rows)

    def kv_copy(i, h, d):
        dst = kv_all.at[h, i, mine, :]
        return pltpu.make_async_remote_copy(
            src_ref=kv_own.at[i, :, pl.ds(h * HEAD, HEAD)] if h < local else dst,
            dst_ref=dst,
            send_sem=kv_send,
            recv_sem=kv_recv.at[h],
            **there(sec, lax.rem(ctx + d, n_ctx), tp),
        )

    def section_copy(src, dst, recv_sem):
        return pltpu.make_async_remote_copy(
            src_ref=src, dst_ref=dst, send_sem=z_send, recv_sem=recv_sem, **there(nxt, ctx, tp)
        )

    for i in range(2):
        section_copy(
            kv_own.at[i, :, pl.ds(local * HEAD, HEAD)], kv_all.at[local, i, mine, :], z_recv.at[0]
        ).start()
    arrived(q_buf.at[:, moved_cols], q_sem.at[0])
    section_copy(q_buf.at[:, moved_cols], q_in, z_recv.at[1]).start()

    @pl.when(early)
    def _():
        pl.semaphore_wait(ctx_in, 1)

    for h in range(local):
        for i in range(2):
            for d in range(1, n_ctx):
                kv_copy(i, h, d).start()
    for h in range(local):
        for i in range(2):
            kv_all[h, i, mine, :] = kv_own[i, :, h * HEAD : (h + 1) * HEAD]

    order_copy.wait()
    row = lax.broadcasted_iota(jnp.int32, (rows, 1), 0)
    row_pos = jnp.where(row < span, order[2 * ctx] * span, order[2 * ctx + 1] * span - span) + row
    lane = lax.broadcasted_iota(jnp.int32, (1, keys), 1)
    key_pos = lane
    for j in range(keys // span):
        key_pos = jnp.where(
            (lane >= j * span) & (lane < (j + 1) * span), lane + (order[j] - j) * span, key_pos
        )
    bias[...] = jnp.where(key_pos <= row_pos, jnp.float32(0.0), jnp.float32(NEG))

    sent = local * per_kv
    late = 2
    scale = math.log2(math.e) / math.sqrt(HEAD)

    def out_copy(c, t):
        return pltpu.make_async_remote_copy(
            src_ref=o_buf.at[c, pl.ds(pl.multiple_of(t * out_rows, out_rows), out_rows), :],
            dst_ref=out_hbm.at[0, :, lanes(tp * q_cols + c * chunk_cols, chunk_cols)],
            send_sem=o_send,
            recv_sem=o_recv,
            **there(nxt, ctx, t),
        )

    def moved_out(c, d):
        t = lax.rem(tp + d, n_tp)
        src = o_buf.at[c, pl.ds(pl.multiple_of(t * out_rows, out_rows), out_rows), :]
        dst = out_hbm.at[0, :, lanes(tp * q_cols + c * chunk_cols, chunk_cols)]
        if d == 0:
            return pltpu.make_async_copy(src, dst, m_own)
        return pltpu.make_async_remote_copy(
            src_ref=src,
            dst_ref=dst,
            send_sem=m_send,
            recv_sem=m_recv,
            **there(sec, ctx, t),
        )

    for h in range(kv_heads):
        if h == 0:
            @pl.when(early)
            def _():
                pl.semaphore_wait(tp_in, 1)
                greet_tp()

            pl.semaphore_wait(next_in, n_tp - 1)

            @pl.when(jnp.logical_not(early))
            def _():
                pl.semaphore_signal(tp_in, inc=1, **there(sec, partner, tp))

            arrived(q_buf.at[:, pl.ds(0, local * group_cols)], q_sem.at[1])
        arrived(kv_all.at[h, :, others, :], kv_recv.at[h])

        def chunk(i, _, h=h):
            c = h * per_kv + i
            q_ref, first = (q_buf, c * g) if h < local else (q_in, i * g)
            q = jnp.concatenate(
                [q_ref[:, lanes((first + j) * HEAD, HEAD)] for j in range(g)], axis=0
            )
            s = lax.dot_general(
                q, kv_all[h, 0], (((1,), (1,)), ((), ())), preferred_element_type=jnp.float32
            )
            s = s.reshape(g, rows, keys) * scale + bias[...][None]
            m = jnp.max(s, axis=-1, keepdims=True)
            p = jnp.exp2(s - m)
            total = jnp.sum(p, axis=-1, keepdims=True)
            o = jnp.dot(
                p.astype(jnp.bfloat16).reshape(g * rows, keys),
                kv_all[h, 1],
                preferred_element_type=jnp.float32,
            ).reshape(g, rows, HEAD)
            o = (o / total).astype(jnp.bfloat16)
            for j in range(g):
                o_buf[c, :, j * HEAD : (j + 1) * HEAD] = o[j]
            if h < local:
                out_copy(c, 0).start()

                @pl.when(c >= late)
                def _():
                    for t in range(1, n_tp):
                        out_copy(c - late, t).start()
            else:
                for d in range(n_tp):
                    moved_out(c, d).start()
            return 0

        lax.fori_loop(0, per_kv, chunk, 0)
        if h == local - 1:
            for c in range(max(sent - late, 0), sent):
                for t in range(1, n_tp):
                    out_copy(c, t).start()
        if h == 0:
            arrived(kv_all.at[local, :, mine, :], z_recv.at[0])
            for i in range(2):
                for d in range(1, n_ctx):
                    kv_copy(i, local, d).start()
        if h == local - 1:
            arrived(q_in, z_recv.at[1])

    kept = chunks - sent
    left(q_buf.at[:, pl.ds(0, group_cols + 2 * HEAD)], z_send)
    left(kv_all.at[:, :, others, :], kv_send)
    arrived(out_hbm.at[0, :, pl.ds(0, kept * chunk_cols)], m_own)
    if n_tp > 1:
        moved = out_hbm.at[0, :, pl.ds(0, (n_tp - 1) * kept * chunk_cols)]
        left(moved, m_send)
        arrived(moved, m_recv)
    left(q_buf.at[:, pl.ds(0, sent * chunk_cols)], o_send)
    arrived(out_hbm.at[0, :, pl.ds(0, n_tp * sent * chunk_cols)], o_recv)


def shards(n_sec, n_ctx, n_tp, queries, keys, values, span_order):
    rows, q_cols, kv_cols = queries.shape[1], queries.shape[2], keys.shape[2]
    kv_heads = kv_cols // HEAD
    group = q_cols // kv_cols
    g = math.gcd(group, 4)
    chunks = q_cols // (g * HEAD)
    all_rows = rows * n_ctx
    dma = pltpu.SemaphoreType.DMA
    any_spec = pl.BlockSpec(memory_space=pl.ANY)
    return pl.pallas_call(
        functools.partial(kernel, n_sec, n_ctx, n_tp, g),
        out_shape=pltpu.VMEM((1, rows // n_tp, q_cols * n_tp), jnp.bfloat16),
        in_specs=[any_spec] * 4,
        out_specs=any_spec,
        scratch_shapes=[
            pltpu.VMEM((rows, q_cols), jnp.bfloat16),
            pltpu.VMEM((rows, group * HEAD), jnp.bfloat16),
            pltpu.VMEM((2, rows, kv_cols), jnp.bfloat16),
            pltpu.VMEM((kv_heads, 2, all_rows, HEAD), jnp.bfloat16),
            pltpu.VMEM((chunks, rows, g * HEAD), jnp.bfloat16),
            pltpu.VMEM((rows, all_rows), jnp.float32),
            pltpu.SMEM(span_order.shape, jnp.int32),
            dma((2,)),
            dma,
            dma,
            dma,
            dma((kv_heads,)),
            dma,
            dma((2,)),
            *[dma] * 5,
            *[pltpu.SemaphoreType.REGULAR] * 3,
        ],
        compiler_params=pltpu.CompilerParams(collective_id=0, has_side_effects=True),
    )(queries, keys, values, span_order)


def solution(mesh):
    sizes = [mesh.shape[axis] for axis in ("section", "ctx", "tp")]
    placed = P("section", "ctx", "tp")
    return jax.shard_map(
        functools.partial(shards, *sizes),
        mesh=mesh,
        in_specs=(placed, placed, placed, P()),
        out_specs=P("section", ("ctx", "tp"), None),
        check_vma=False,
    )
```

```python
import functools
import math

import jax
import jax.numpy as jnp
from jax import lax
from jax.experimental import pallas as pl
from jax.experimental.pallas import tpu as pltpu
from jax.sharding import PartitionSpec as P

HEAD = 128
MESH = pl.DeviceIdType.MESH
NEG = -1e30
EARLY = 1


def lanes(start, size):
    return pl.ds(pl.multiple_of(start, HEAD), size)


def kernel(
    n_sec, n_ctx, n_tp, heads_per_chunk,
    q_hbm, k_hbm, v_hbm, order_hbm, out_hbm,
    q_buf, q_in, kv_own, kv_all, o_buf, relayed, bias, order,
    q_sem, own_sem, order_sem, kv_send, kv_recv, z_send, z_recv,
    o_send, o_recv, m_send, m_recv, m_own, r_send, r_recv, ctx_in, tp_in, next_in,
):
    sec, ctx, tp = lax.axis_index("section"), lax.axis_index("ctx"), lax.axis_index("tp")
    rows, q_cols = q_hbm.shape[1], q_hbm.shape[2]
    kv_heads = k_hbm.shape[2] // HEAD
    group = q_cols // k_hbm.shape[2]
    g = heads_per_chunk
    chunk_cols = g * HEAD
    chunks = q_cols // chunk_cols
    per_kv = group // g
    out_rows = rows // n_tp
    keys = rows * n_ctx
    span = rows // 2
    local = kv_heads - 1
    group_cols = group * HEAD
    moved_cols = pl.ds(local * group_cols, group_cols)
    nxt, prv = lax.rem(sec + 1, n_sec), lax.rem(sec + n_sec - 1, n_sec)

    def there(s, c, t):
        return dict(device_id=(s, c, t), device_id_type=MESH)

    early = lax.rem(ctx, 2) == EARLY
    partner = ctx + 1 - 2 * lax.rem(ctx, 2)
    barrier = pltpu.get_barrier_semaphore()
    pl.semaphore_signal(barrier, inc=1, **there(prv, ctx, tp))
    for d in range(1, n_ctx):
        peer = lax.rem(ctx + d, n_ctx)

        @pl.when(lax.rem(peer, 2) != EARLY)
        def _():
            pl.semaphore_signal(barrier, inc=1, **there(sec, peer, tp))

    @pl.when(jnp.logical_not(early))
    def _():
        for d in range(1, n_tp):
            pl.semaphore_signal(barrier, inc=1, **there(sec, ctx, lax.rem(tp + d, n_tp)))

    def arrived(ref, sem):
        pltpu.make_async_copy(ref, ref, sem).wait()

    def left(ref, sem):
        pltpu.make_async_remote_copy(
            src_ref=ref, dst_ref=ref, send_sem=sem, recv_sem=sem, **there(nxt, ctx, tp)
        ).wait_send()

    for i, src in enumerate((k_hbm, v_hbm)):
        pltpu.make_async_copy(src.at[0], kv_own.at[i], own_sem).start()
    order_copy = pltpu.make_async_copy(order_hbm, order, order_sem)
    order_copy.start()
    kept_cols = pl.ds(0, local * group_cols)
    pltpu.make_async_copy(q_hbm.at[0, :, kept_cols], q_buf, q_sem).start()

    def greet_tp():
        for d in range(1, n_tp):
            pl.semaphore_signal(next_in, inc=1, **there(sec, ctx, lax.rem(tp + d, n_tp)))

    pl.semaphore_wait(barrier, jnp.where(early, 1, n_ctx + n_tp - 1))

    @pl.when(jnp.logical_not(early))
    def _():
        pl.semaphore_signal(ctx_in, inc=1, **there(sec, partner, tp))
        greet_tp()

    others = pl.ds(0, keys - rows)
    mine = pl.ds(pl.multiple_of(ctx * rows, rows), rows)

    def kv_copy(i, h, d):
        dst = kv_all.at[h, i, mine, :]
        return pltpu.make_async_remote_copy(
            src_ref=kv_own.at[i, :, pl.ds(h * HEAD, HEAD)] if h < local else dst,
            dst_ref=dst,
            send_sem=kv_send,
            recv_sem=kv_recv.at[h],
            **there(sec, lax.rem(ctx + d, n_ctx), tp),
        )

    def section_copy(src, dst, recv_sem):
        return pltpu.make_async_remote_copy(
            src_ref=src, dst_ref=dst, send_sem=z_send, recv_sem=recv_sem, **there(nxt, ctx, tp)
        )

    section_copy(q_hbm.at[0, :, moved_cols], q_in, z_recv.at[1]).start()
    for i, src in enumerate((k_hbm, v_hbm)):
        section_copy(
            src.at[0, :, pl.ds(local * HEAD, HEAD)], kv_all.at[local, i, mine, :], z_recv.at[0]
        ).start()
    arrived(kv_own, own_sem)

    @pl.when(early)
    def _():
        pl.semaphore_wait(ctx_in, 1)

    for h in range(local):
        for i in range(2):
            for d in range(1, n_ctx):
                kv_copy(i, h, d).start()
    for h in range(local):
        for i in range(2):
            kv_all[h, i, mine, :] = kv_own[i, :, h * HEAD : (h + 1) * HEAD]

    order_copy.wait()
    row = lax.broadcasted_iota(jnp.int32, (rows, 1), 0)
    row_pos = jnp.where(row < span, order[2 * ctx] * span, order[2 * ctx + 1] * span - span) + row
    lane = lax.broadcasted_iota(jnp.int32, (1, keys), 1)
    key_pos = lane
    for j in range(keys // span):
        key_pos = jnp.where(
            (lane >= j * span) & (lane < (j + 1) * span), lane + (order[j] - j) * span, key_pos
        )
    bias[...] = jnp.where(key_pos <= row_pos, jnp.float32(0.0), jnp.float32(NEG))

    sent = local * per_kv
    late = 2
    scale = math.log2(math.e) / math.sqrt(HEAD)

    def out_copy(c, t):
        return pltpu.make_async_remote_copy(
            src_ref=o_buf.at[c, pl.ds(pl.multiple_of(t * out_rows, out_rows), out_rows), :],
            dst_ref=out_hbm.at[0, :, lanes(tp * q_cols + c * chunk_cols, chunk_cols)],
            send_sem=o_send,
            recv_sem=o_recv,
            **there(nxt, ctx, t),
        )

    relay_rows = relayed.shape[0]
    relays = n_tp > 1 and n_ctx % 4 == 0
    gives = jnp.logical_and(lax.rem(ctx, 4) == 1, tp == 0)
    takes = jnp.logical_and(lax.rem(ctx, 4) == 2, tp == 1)

    def piece(c, first, size):
        return o_buf.at[c, pl.ds(out_rows + first, size), :]

    def give():
        pltpu.make_async_remote_copy(
            src_ref=piece(0, 0, relay_rows),
            dst_ref=relayed,
            send_sem=o_send,
            recv_sem=r_recv,
            **there(sec, lax.rem(ctx + 1, n_ctx), 1),
        ).start()

    def send_rest():
        rest = pl.ds(relay_rows, out_rows - relay_rows)
        pltpu.make_async_remote_copy(
            src_ref=piece(0, relay_rows, out_rows - relay_rows),
            dst_ref=out_hbm.at[0, rest, lanes(tp * q_cols, chunk_cols)],
            send_sem=o_send,
            recv_sem=o_recv,
            **there(nxt, ctx, 1),
        ).start()

    def pass_on():
        return pltpu.make_async_remote_copy(
            src_ref=relayed,
            dst_ref=out_hbm.at[0, pl.ds(0, relay_rows), pl.ds(0, chunk_cols)],
            send_sem=r_send,
            recv_sem=o_recv,
            **there(nxt, lax.rem(ctx + n_ctx - 1, n_ctx), 1),
        )

    def send_late(c):
        if not relays:
            for t in range(1, n_tp):
                out_copy(c, t).start()
            return
        given = jnp.logical_and(gives, c == 0)
        pl.when(given)(send_rest)

        @pl.when(jnp.logical_not(given))
        def _():
            out_copy(c, 1).start()

        for t in range(2, n_tp):
            out_copy(c, t).start()

    def moved_out(c, d):
        t = lax.rem(tp + d, n_tp)
        src = o_buf.at[c, pl.ds(pl.multiple_of(t * out_rows, out_rows), out_rows), :]
        dst = out_hbm.at[0, :, lanes(tp * q_cols + c * chunk_cols, chunk_cols)]
        if d == 0:
            return pltpu.make_async_copy(src, dst, m_own)
        return pltpu.make_async_remote_copy(
            src_ref=src,
            dst_ref=dst,
            send_sem=m_send,
            recv_sem=m_recv,
            **there(sec, ctx, t),
        )

    for h in range(kv_heads):
        if h == 0:
            @pl.when(early)
            def _():
                pl.semaphore_wait(tp_in, 1)
                greet_tp()

            pl.semaphore_wait(next_in, n_tp - 1)

            @pl.when(jnp.logical_not(early))
            def _():
                pl.semaphore_signal(tp_in, inc=1, **there(sec, partner, tp))

            arrived(q_buf, q_sem)
        arrived(kv_all.at[h, :, others, :], kv_recv.at[h])

        def chunk(i, _, h=h):
            c = h * per_kv + i
            q_ref, first = (q_buf, c * g) if h < local else (q_in, i * g)
            q = jnp.concatenate(
                [q_ref[:, lanes((first + j) * HEAD, HEAD)] for j in range(g)], axis=0
            )
            s = lax.dot_general(
                q, kv_all[h, 0], (((1,), (1,)), ((), ())), preferred_element_type=jnp.float32
            )
            s = s.reshape(g, rows, keys) * scale + bias[...][None]
            m = jnp.max(s, axis=-1, keepdims=True)
            p = jnp.exp2(s - m)
            total = jnp.sum(p, axis=-1, keepdims=True)
            o = jnp.dot(
                p.astype(jnp.bfloat16).reshape(g * rows, keys),
                kv_all[h, 1],
                preferred_element_type=jnp.float32,
            ).reshape(g, rows, HEAD)
            o = (o / total).astype(jnp.bfloat16)
            for j in range(g):
                o_buf[c, :, j * HEAD : (j + 1) * HEAD] = o[j]
            if h < local:
                if relays:
                    pl.when(jnp.logical_and(gives, c == 0))(give)
                out_copy(c, 0).start()

                @pl.when(c >= late)
                def _():
                    send_late(c - late)
            else:
                for d in range(n_tp):
                    moved_out(c, d).start()
            return 0

        lax.fori_loop(0, per_kv, chunk, 0)
        if h == local - 1:
            if relays:
                @pl.when(takes)
                def _():
                    arrived(relayed, r_recv)
                    pass_on().start()

            for c in range(max(sent - late, 0), sent):
                send_late(c)
        if h == min(1, local - 1):
            arrived(kv_all.at[local, :, mine, :], z_recv.at[0])
            for i in range(2):
                for d in range(1, n_ctx):
                    kv_copy(i, local, d).start()
        if h == local - 1:
            arrived(q_in, z_recv.at[1])

    kept = chunks - sent
    left(q_in, z_send)
    left(kv_all.at[0, :, mine, :], z_send)
    left(kv_all.at[:, :, others, :], kv_send)
    arrived(out_hbm.at[0, :, pl.ds(0, kept * chunk_cols)], m_own)
    if n_tp > 1:
        moved = out_hbm.at[0, :, pl.ds(0, (n_tp - 1) * kept * chunk_cols)]
        left(moved, m_send)
        arrived(moved, m_recv)
    left(q_buf, o_send)
    if relays:
        @pl.when(takes)
        def _():
            pass_on().wait_send()

    arrived(out_hbm.at[0, :, pl.ds(0, n_tp * sent * chunk_cols)], o_recv)


def shards(n_sec, n_ctx, n_tp, queries, keys, values, span_order):
    rows, q_cols, kv_cols = queries.shape[1], queries.shape[2], keys.shape[2]
    kv_heads = kv_cols // HEAD
    group = q_cols // kv_cols
    g = math.gcd(group, 4)
    chunks = q_cols // (g * HEAD)
    all_rows = rows * n_ctx
    dma = pltpu.SemaphoreType.DMA
    any_spec = pl.BlockSpec(memory_space=pl.ANY)
    return pl.pallas_call(
        functools.partial(kernel, n_sec, n_ctx, n_tp, g),
        out_shape=pltpu.VMEM((1, rows // n_tp, q_cols * n_tp), jnp.bfloat16),
        in_specs=[any_spec] * 4,
        out_specs=any_spec,
        scratch_shapes=[
            pltpu.VMEM((rows, q_cols - group * HEAD), jnp.bfloat16),
            pltpu.VMEM((rows, group * HEAD), jnp.bfloat16),
            pltpu.VMEM((2, rows, kv_cols), jnp.bfloat16),
            pltpu.VMEM((kv_heads, 2, all_rows, HEAD), jnp.bfloat16),
            pltpu.VMEM((chunks, rows, g * HEAD), jnp.bfloat16),
            pltpu.VMEM((3 * rows // n_tp // 4, g * HEAD), jnp.bfloat16),
            pltpu.VMEM((rows, all_rows), jnp.float32),
            pltpu.SMEM(span_order.shape, jnp.int32),
            dma,
            dma,
            dma,
            dma,
            dma((kv_heads,)),
            dma,
            dma((2,)),
            *[dma] * 7,
            *[pltpu.SemaphoreType.REGULAR] * 3,
        ],
        compiler_params=pltpu.CompilerParams(collective_id=0, has_side_effects=True),
    )(queries, keys, values, span_order)


def solution(mesh):
    sizes = [mesh.shape[axis] for axis in ("section", "ctx", "tp")]
    placed = P("section", "ctx", "tp")
    return jax.shard_map(
        functools.partial(shards, *sizes),
        mesh=mesh,
        in_specs=(placed, placed, placed, P()),
        out_specs=P("section", ("ctx", "tp"), None),
        check_vma=False,
    )
```

```python
import functools
import math

import jax
import jax.numpy as jnp
from jax import lax
from jax.experimental import pallas as pl
from jax.experimental.pallas import tpu as pltpu
from jax.sharding import PartitionSpec as P

HEAD = 128
MESH = pl.DeviceIdType.MESH
NEG = -1e30
EARLY = 1


def lanes(start, size):
    return pl.ds(pl.multiple_of(start, HEAD), size)


def kernel(
    n_sec, n_ctx, n_tp, heads_per_chunk,
    q_hbm, k_hbm, v_hbm, order_hbm, out_hbm,
    q_buf, q_in, kv_own, kv_all, o_buf, relayed, bias, order,
    q_sem, own_sem, order_sem, kv_send, kv_recv, z_send, z_recv,
    o_send, o_recv, m_send, m_recv, m_own, r_send, r_recv, ctx_in, tp_in, next_in,
):
    sec, ctx, tp = lax.axis_index("section"), lax.axis_index("ctx"), lax.axis_index("tp")
    rows, q_cols = q_hbm.shape[1], q_hbm.shape[2]
    kv_heads = k_hbm.shape[2] // HEAD
    group = q_cols // k_hbm.shape[2]
    g = heads_per_chunk
    chunk_cols = g * HEAD
    chunks = q_cols // chunk_cols
    per_kv = group // g
    out_rows = rows // n_tp
    keys = rows * n_ctx
    span = rows // 2
    local = kv_heads - 1
    group_cols = group * HEAD
    moved_cols = pl.ds(local * group_cols, group_cols)
    nxt, prv = lax.rem(sec + 1, n_sec), lax.rem(sec + n_sec - 1, n_sec)

    def there(s, c, t):
        return dict(device_id=(s, c, t), device_id_type=MESH)

    early = lax.rem(ctx, 2) == EARLY
    partner = ctx + 1 - 2 * lax.rem(ctx, 2)
    barrier = pltpu.get_barrier_semaphore()
    pl.semaphore_signal(barrier, inc=1, **there(prv, ctx, tp))
    for d in range(1, n_ctx):
        peer = lax.rem(ctx + d, n_ctx)

        @pl.when(lax.rem(peer, 2) != EARLY)
        def _():
            pl.semaphore_signal(barrier, inc=1, **there(sec, peer, tp))

    @pl.when(jnp.logical_not(early))
    def _():
        for d in range(1, n_tp):
            pl.semaphore_signal(barrier, inc=1, **there(sec, ctx, lax.rem(tp + d, n_tp)))

    def arrived(ref, sem):
        pltpu.make_async_copy(ref, ref, sem).wait()

    def left(ref, sem):
        pltpu.make_async_remote_copy(
            src_ref=ref, dst_ref=ref, send_sem=sem, recv_sem=sem, **there(nxt, ctx, tp)
        ).wait_send()

    kept_cols = pl.ds(0, local * group_cols)
    order_copy = pltpu.make_async_copy(order_hbm, order, order_sem)

    def load():
        for i, src in enumerate((k_hbm, v_hbm)):
            pltpu.make_async_copy(src.at[0], kv_own.at[i], own_sem).start()
        order_copy.start()
        pltpu.make_async_copy(q_hbm.at[0, :, kept_cols], q_buf, q_sem).start()

    pl.when(jnp.logical_not(early))(load)

    def greet_tp():
        for d in range(1, n_tp):
            pl.semaphore_signal(next_in, inc=1, **there(sec, ctx, lax.rem(tp + d, n_tp)))

    pl.semaphore_wait(barrier, jnp.where(early, 1, n_ctx + n_tp - 1))

    @pl.when(jnp.logical_not(early))
    def _():
        pl.semaphore_signal(ctx_in, inc=1, **there(sec, partner, tp))
        greet_tp()

    others = pl.ds(0, keys - rows)
    mine = pl.ds(pl.multiple_of(ctx * rows, rows), rows)

    def kv_copy(i, h, d):
        dst = kv_all.at[h, i, mine, :]
        return pltpu.make_async_remote_copy(
            src_ref=kv_own.at[i, :, pl.ds(h * HEAD, HEAD)] if h < local else dst,
            dst_ref=dst,
            send_sem=kv_send,
            recv_sem=kv_recv.at[h],
            **there(sec, lax.rem(ctx + d, n_ctx), tp),
        )

    def section_copy(src, dst, recv_sem):
        return pltpu.make_async_remote_copy(
            src_ref=src, dst_ref=dst, send_sem=z_send, recv_sem=recv_sem, **there(nxt, ctx, tp)
        )

    section_copy(q_hbm.at[0, :, moved_cols], q_in, z_recv.at[1]).start()
    for i, src in enumerate((k_hbm, v_hbm)):
        section_copy(
            src.at[0, :, pl.ds(local * HEAD, HEAD)], kv_all.at[local, i, mine, :], z_recv.at[0]
        ).start()
    pl.when(early)(load)
    arrived(kv_own, own_sem)

    @pl.when(early)
    def _():
        pl.semaphore_wait(ctx_in, 1)

    for h in range(local):
        for i in range(2):
            for d in range(1, n_ctx):
                kv_copy(i, h, d).start()
    for h in range(local):
        for i in range(2):
            kv_all[h, i, mine, :] = kv_own[i, :, h * HEAD : (h + 1) * HEAD]

    order_copy.wait()
    row = lax.broadcasted_iota(jnp.int32, (rows, 1), 0)
    row_pos = jnp.where(row < span, order[2 * ctx] * span, order[2 * ctx + 1] * span - span) + row
    lane = lax.broadcasted_iota(jnp.int32, (1, keys), 1)
    key_pos = lane
    for j in range(keys // span):
        key_pos = jnp.where(
            (lane >= j * span) & (lane < (j + 1) * span), lane + (order[j] - j) * span, key_pos
        )
    bias[...] = jnp.where(key_pos <= row_pos, jnp.float32(0.0), jnp.float32(NEG))

    sent = local * per_kv
    late = 4
    scale = math.log2(math.e) / math.sqrt(HEAD)

    def out_copy(c, t):
        return pltpu.make_async_remote_copy(
            src_ref=o_buf.at[c, pl.ds(pl.multiple_of(t * out_rows, out_rows), out_rows), :],
            dst_ref=out_hbm.at[0, :, lanes(tp * q_cols + c * chunk_cols, chunk_cols)],
            send_sem=o_send,
            recv_sem=o_recv,
            **there(nxt, ctx, t),
        )

    n_relay = relayed.shape[0]
    relays = n_tp > 1 and n_ctx % 4 == 0
    gives = jnp.logical_and(lax.rem(ctx, 4) == 1, tp == 0)
    takes = jnp.logical_and(lax.rem(ctx, 4) == 2, tp == 1)

    def give(c):
        pltpu.make_async_remote_copy(
            src_ref=o_buf.at[c, pl.ds(out_rows, out_rows), :],
            dst_ref=relayed.at[c],
            send_sem=o_send,
            recv_sem=r_recv,
            **there(sec, lax.rem(ctx + 1, n_ctx), 1),
        ).start()

    def pass_on(c):
        return pltpu.make_async_remote_copy(
            src_ref=relayed.at[c],
            dst_ref=out_hbm.at[0, :, pl.ds(c * chunk_cols, chunk_cols)],
            send_sem=r_send,
            recv_sem=o_recv,
            **there(nxt, lax.rem(ctx + n_ctx - 1, n_ctx), 1),
        )

    def send_late(c):
        if relays:
            @pl.when(jnp.logical_not(jnp.logical_and(gives, c < n_relay)))
            def _():
                out_copy(c, 1).start()

        for t in range(2 if relays else 1, n_tp):
            out_copy(c, t).start()

    def moved_out(c, d):
        t = lax.rem(tp + d, n_tp)
        src = o_buf.at[c, pl.ds(pl.multiple_of(t * out_rows, out_rows), out_rows), :]
        dst = out_hbm.at[0, :, lanes(tp * q_cols + c * chunk_cols, chunk_cols)]
        if d == 0:
            return pltpu.make_async_copy(src, dst, m_own)
        return pltpu.make_async_remote_copy(
            src_ref=src,
            dst_ref=dst,
            send_sem=m_send,
            recv_sem=m_recv,
            **there(sec, ctx, t),
        )

    for h in range(kv_heads):
        if h == 0:
            @pl.when(early)
            def _():
                pl.semaphore_wait(tp_in, 1)
                greet_tp()

            pl.semaphore_wait(next_in, n_tp - 1)

            @pl.when(jnp.logical_not(early))
            def _():
                pl.semaphore_signal(tp_in, inc=1, **there(sec, partner, tp))

            arrived(q_buf, q_sem)
        arrived(kv_all.at[h, :, others, :], kv_recv.at[h])

        def chunk(i, _, h=h):
            c = h * per_kv + i
            q_ref, first = (q_buf, c * g) if h < local else (q_in, i * g)
            q = jnp.concatenate(
                [q_ref[:, lanes((first + j) * HEAD, HEAD)] for j in range(g)], axis=0
            )
            s = lax.dot_general(
                q, kv_all[h, 0], (((1,), (1,)), ((), ())), preferred_element_type=jnp.float32
            )
            s = s.reshape(g, rows, keys) * scale + bias[...][None]
            m = jnp.max(s, axis=-1, keepdims=True)
            p = jnp.exp2(s - m)
            total = jnp.sum(p, axis=-1, keepdims=True)
            o = jnp.dot(
                p.astype(jnp.bfloat16).reshape(g * rows, keys),
                kv_all[h, 1],
                preferred_element_type=jnp.float32,
            ).reshape(g, rows, HEAD)
            o = (o / total).astype(jnp.bfloat16)
            for j in range(g):
                o_buf[c, :, j * HEAD : (j + 1) * HEAD] = o[j]
            if h < local:
                if relays:
                    @pl.when(jnp.logical_and(gives, c < n_relay))
                    def _():
                        give(c)

                out_copy(c, 0).start()

                @pl.when(c >= late)
                def _():
                    send_late(c - late)
            else:
                for d in range(n_tp):
                    moved_out(c, d).start()
            return 0

        lax.fori_loop(0, per_kv, chunk, 0)
        if h == local - 1:
            if relays:
                @pl.when(takes)
                def _():
                    arrived(relayed, r_recv)
                    for c in range(n_relay):
                        pass_on(c).start()

            for c in range(max(sent - late, 0), sent):
                send_late(c)
        if h == min(1, local - 1):
            arrived(kv_all.at[local, :, mine, :], z_recv.at[0])
            for i in range(2):
                for d in range(1, n_ctx):
                    kv_copy(i, local, d).start()
        if h == local - 1:
            arrived(q_in, z_recv.at[1])

    kept = chunks - sent
    left(q_in, z_send)
    left(kv_all.at[0, :, mine, :], z_send)
    left(kv_all.at[:, :, others, :], kv_send)
    arrived(out_hbm.at[0, :, pl.ds(0, kept * chunk_cols)], m_own)
    if n_tp > 1:
        moved = out_hbm.at[0, :, pl.ds(0, (n_tp - 1) * kept * chunk_cols)]
        left(moved, m_send)
        arrived(moved, m_recv)
    left(q_buf, o_send)
    if relays:
        @pl.when(takes)
        def _():
            left(relayed, r_send)

    arrived(out_hbm.at[0, :, pl.ds(0, n_tp * sent * chunk_cols)], o_recv)


def shards(n_sec, n_ctx, n_tp, queries, keys, values, span_order):
    rows, q_cols, kv_cols = queries.shape[1], queries.shape[2], keys.shape[2]
    kv_heads = kv_cols // HEAD
    group = q_cols // kv_cols
    g = math.gcd(group, 2)
    relay = 1
    chunks = q_cols // (g * HEAD)
    all_rows = rows * n_ctx
    dma = pltpu.SemaphoreType.DMA
    any_spec = pl.BlockSpec(memory_space=pl.ANY)
    return pl.pallas_call(
        functools.partial(kernel, n_sec, n_ctx, n_tp, g),
        out_shape=pltpu.VMEM((1, rows // n_tp, q_cols * n_tp), jnp.bfloat16),
        in_specs=[any_spec] * 4,
        out_specs=any_spec,
        scratch_shapes=[
            pltpu.VMEM((rows, q_cols - group * HEAD), jnp.bfloat16),
            pltpu.VMEM((rows, group * HEAD), jnp.bfloat16),
            pltpu.VMEM((2, rows, kv_cols), jnp.bfloat16),
            pltpu.VMEM((kv_heads, 2, all_rows, HEAD), jnp.bfloat16),
            pltpu.VMEM((chunks, rows, g * HEAD), jnp.bfloat16),
            pltpu.VMEM((relay, rows // n_tp, g * HEAD), jnp.bfloat16),
            pltpu.VMEM((rows, all_rows), jnp.float32),
            pltpu.SMEM(span_order.shape, jnp.int32),
            dma,
            dma,
            dma,
            dma,
            dma((kv_heads,)),
            dma,
            dma((2,)),
            *[dma] * 7,
            *[pltpu.SemaphoreType.REGULAR] * 3,
        ],
        compiler_params=pltpu.CompilerParams(collective_id=0, has_side_effects=True),
    )(queries, keys, values, span_order)


def solution(mesh):
    sizes = [mesh.shape[axis] for axis in ("section", "ctx", "tp")]
    placed = P("section", "ctx", "tp")
    return jax.shard_map(
        functools.partial(shards, *sizes),
        mesh=mesh,
        in_specs=(placed, placed, placed, P()),
        out_specs=P("section", ("ctx", "tp"), None),
        check_vma=False,
    )
```

```python
import functools
import math

import jax
import jax.numpy as jnp
from jax import lax
from jax.experimental import pallas as pl
from jax.experimental.pallas import tpu as pltpu
from jax.sharding import PartitionSpec as P

HEAD = 128
MESH = pl.DeviceIdType.MESH
NEG = -1e30
EARLY = 1


def lanes(start, size):
    return pl.ds(pl.multiple_of(start, HEAD), size)


def kernel(
    n_sec, n_ctx, n_tp, heads_per_chunk,
    q_hbm, k_hbm, v_hbm, order_hbm, out_hbm,
    q_buf, q_in, kv_own, kv_all, o_buf, relayed, bias, order,
    q_sem, own_sem, order_sem, sends, kv_recv, z_recv, o_recv, r_recv, pair_in, next_in,
):
    sec, ctx, tp = lax.axis_index("section"), lax.axis_index("ctx"), lax.axis_index("tp")
    rows, q_cols = q_hbm.shape[1], q_hbm.shape[2]
    kv_heads = k_hbm.shape[2] // HEAD
    group = q_cols // k_hbm.shape[2]
    g = heads_per_chunk
    chunk_cols = g * HEAD
    chunks = q_cols // chunk_cols
    per_kv = group // g
    out_rows = rows // n_tp
    keys = rows * n_ctx
    span = rows // 2
    local = kv_heads - 1
    group_cols = group * HEAD
    moved_cols = pl.ds(local * group_cols, group_cols)
    nxt, prv = lax.rem(sec + 1, n_sec), lax.rem(sec + n_sec - 1, n_sec)

    def there(s, c, t):
        return dict(device_id=(s, c, t), device_id_type=MESH)

    early = lax.rem(ctx, 2) == EARLY
    partner = ctx + 1 - 2 * lax.rem(ctx, 2)
    barrier = pltpu.get_barrier_semaphore()
    pl.semaphore_signal(barrier, inc=1, **there(prv, ctx, tp))
    for d in range(1, n_ctx):
        peer = lax.rem(ctx + d, n_ctx)

        @pl.when(lax.rem(peer, 2) != EARLY)
        def _():
            pl.semaphore_signal(barrier, inc=1, **there(sec, peer, tp))

    @pl.when(jnp.logical_not(early))
    def _():
        for d in range(1, n_tp):
            pl.semaphore_signal(barrier, inc=1, **there(sec, ctx, lax.rem(tp + d, n_tp)))

    def arrived(ref, sem):
        pltpu.make_async_copy(ref, ref, sem).wait()

    def left(ref, sem):
        pltpu.make_async_remote_copy(
            src_ref=ref, dst_ref=ref, send_sem=sem, recv_sem=sem, **there(nxt, ctx, tp)
        ).wait_send()

    kept_cols = pl.ds(0, local * group_cols)
    order_copy = pltpu.make_async_copy(order_hbm, order, order_sem)

    def load():
        for i, src in enumerate((k_hbm, v_hbm)):
            pltpu.make_async_copy(src.at[0], kv_own.at[i], own_sem).start()
        order_copy.start()
        pltpu.make_async_copy(q_hbm.at[0, :, kept_cols], q_buf, q_sem).start()

    pl.when(jnp.logical_not(early))(load)

    def greet_tp():
        for d in range(1, n_tp):
            pl.semaphore_signal(next_in, inc=1, **there(sec, ctx, lax.rem(tp + d, n_tp)))

    pl.semaphore_wait(barrier, jnp.where(early, 1, n_ctx + n_tp - 1))

    @pl.when(jnp.logical_not(early))
    def _():
        pl.semaphore_signal(pair_in, inc=1, **there(sec, partner, tp))
        greet_tp()

    others = pl.ds(0, keys - rows)
    mine = pl.ds(pl.multiple_of(ctx * rows, rows), rows)

    def kv_copy(i, h, d):
        dst = kv_all.at[h, i, mine, :]
        return pltpu.make_async_remote_copy(
            src_ref=kv_own.at[i, :, pl.ds(h * HEAD, HEAD)] if h < local else dst,
            dst_ref=dst,
            send_sem=sends,
            recv_sem=kv_recv.at[h],
            **there(sec, lax.rem(ctx + d, n_ctx), tp),
        )

    def section_copy(src, dst, recv_sem):
        return pltpu.make_async_remote_copy(
            src_ref=src, dst_ref=dst, send_sem=sends, recv_sem=recv_sem, **there(nxt, ctx, tp)
        )

    section_copy(q_hbm.at[0, :, moved_cols], q_in, z_recv.at[1]).start()
    for i, src in enumerate((k_hbm, v_hbm)):
        section_copy(
            src.at[0, :, pl.ds(local * HEAD, HEAD)], kv_all.at[local, i, mine, :], z_recv.at[0]
        ).start()
    pl.when(early)(load)
    arrived(kv_own, own_sem)

    @pl.when(early)
    def _():
        pl.semaphore_wait(pair_in, 1)

    for h in range(local):
        for i in range(2):
            for d in range(1, n_ctx):
                kv_copy(i, h, d).start()
    for h in range(local):
        for i in range(2):
            kv_all[h, i, mine, :] = kv_own[i, :, h * HEAD : (h + 1) * HEAD]

    order_copy.wait()
    row = lax.broadcasted_iota(jnp.int32, (rows, 1), 0)
    row_pos = jnp.where(row < span, order[2 * ctx] * span, order[2 * ctx + 1] * span - span) + row
    lane = lax.broadcasted_iota(jnp.int32, (1, keys), 1)
    key_pos = lane
    for j in range(keys // span):
        key_pos = jnp.where(
            (lane >= j * span) & (lane < (j + 1) * span), lane + (order[j] - j) * span, key_pos
        )
    bias[...] = jnp.where(key_pos <= row_pos, jnp.float32(0.0), jnp.float32(NEG))

    sent = local * per_kv
    late = 4
    scale = math.log2(math.e) / math.sqrt(HEAD)

    def out_copy(c, t):
        return pltpu.make_async_remote_copy(
            src_ref=o_buf.at[c, pl.ds(pl.multiple_of(t * out_rows, out_rows), out_rows), :],
            dst_ref=out_hbm.at[0, :, lanes(tp * q_cols + c * chunk_cols, chunk_cols)],
            send_sem=sends,
            recv_sem=o_recv,
            **there(nxt, ctx, t),
        )

    n_relay = relayed.shape[0]
    relays = n_tp > 1 and n_ctx % 4 == 0
    gives = jnp.logical_and(lax.rem(ctx, 4) == 1, tp == 0)
    takes = jnp.logical_and(lax.rem(ctx, 4) == 2, tp == 1)

    def give(c):
        pltpu.make_async_remote_copy(
            src_ref=o_buf.at[c, pl.ds(out_rows, out_rows), :],
            dst_ref=relayed.at[c],
            send_sem=sends,
            recv_sem=r_recv,
            **there(sec, lax.rem(ctx + 1, n_ctx), 1),
        ).start()

    def pass_on(c):
        return pltpu.make_async_remote_copy(
            src_ref=relayed.at[c],
            dst_ref=out_hbm.at[0, :, pl.ds(c * chunk_cols, chunk_cols)],
            send_sem=sends,
            recv_sem=o_recv,
            **there(nxt, lax.rem(ctx + n_ctx - 1, n_ctx), 1),
        )

    def send_late(c):
        if relays:
            @pl.when(jnp.logical_not(jnp.logical_and(gives, c < n_relay)))
            def _():
                out_copy(c, 1).start()

        for t in range(2 if relays else 1, n_tp):
            out_copy(c, t).start()

    def moved_out(c, d):
        t = lax.rem(tp + d, n_tp)
        src = o_buf.at[c, pl.ds(pl.multiple_of(t * out_rows, out_rows), out_rows), :]
        dst = out_hbm.at[0, :, lanes(tp * q_cols + c * chunk_cols, chunk_cols)]
        if d == 0:
            return pltpu.make_async_copy(src, dst, o_recv)
        return pltpu.make_async_remote_copy(
            src_ref=src,
            dst_ref=dst,
            send_sem=sends,
            recv_sem=o_recv,
            **there(sec, ctx, t),
        )

    for h in range(kv_heads):
        if h == 0:
            @pl.when(early)
            def _():
                pl.semaphore_wait(pair_in, 1)
                greet_tp()

            pl.semaphore_wait(next_in, n_tp - 1)

            @pl.when(jnp.logical_not(early))
            def _():
                pl.semaphore_signal(pair_in, inc=1, **there(sec, partner, tp))

            arrived(q_buf, q_sem)
        arrived(kv_all.at[h, :, others, :], kv_recv.at[h])

        def chunk(i, _, h=h):
            c = h * per_kv + i
            q_ref, first = (q_buf, c * g) if h < local else (q_in, i * g)
            q = jnp.concatenate(
                [q_ref[:, lanes((first + j) * HEAD, HEAD)] for j in range(g)], axis=0
            )
            s = lax.dot_general(
                q, kv_all[h, 0], (((1,), (1,)), ((), ())), preferred_element_type=jnp.float32
            )
            s = s.reshape(g, rows, keys) * scale + bias[...][None]
            m = jnp.max(s, axis=-1, keepdims=True)
            p = jnp.exp2(s - m)
            total = jnp.sum(p, axis=-1, keepdims=True)
            o = jnp.dot(
                p.astype(jnp.bfloat16).reshape(g * rows, keys),
                kv_all[h, 1],
                preferred_element_type=jnp.float32,
            ).reshape(g, rows, HEAD)
            o = (o / total).astype(jnp.bfloat16)
            for j in range(g):
                o_buf[c, :, j * HEAD : (j + 1) * HEAD] = o[j]
            if h < local:
                if relays:
                    @pl.when(jnp.logical_and(gives, c < n_relay))
                    def _():
                        give(c)

                out_copy(c, 0).start()

                @pl.when(c >= late)
                def _():
                    send_late(c - late)
            else:
                for d in range(n_tp):
                    moved_out(c, d).start()
            return 0

        lax.fori_loop(0, per_kv, chunk, 0)
        if h == local - 1:
            if relays:
                @pl.when(takes)
                def _():
                    arrived(relayed, r_recv)
                    for c in range(n_relay):
                        pass_on(c).start()

            for c in range(max(sent - late, 0), sent):
                send_late(c)
        if h == min(1, local - 1):
            arrived(kv_all.at[local, :, mine, :], z_recv.at[0])
            for i in range(2):
                for d in range(1, n_ctx):
                    kv_copy(i, local, d).start()
        if h == local - 1:
            arrived(q_in, z_recv.at[1])

    kept = chunks - sent
    left(q_in, sends)
    left(kv_all.at[0, :, mine, :], sends)
    left(kv_all.at[:, :, others, :], sends)
    if n_tp > 1:
        left(out_hbm.at[0, :, pl.ds(0, (n_tp - 1) * kept * chunk_cols)], sends)
    left(q_buf, sends)
    if relays:
        @pl.when(takes)
        def _():
            left(relayed, sends)

    arrived(out_hbm.at[0], o_recv)


def shards(n_sec, n_ctx, n_tp, queries, keys, values, span_order):
    rows, q_cols, kv_cols = queries.shape[1], queries.shape[2], keys.shape[2]
    kv_heads = kv_cols // HEAD
    group = q_cols // kv_cols
    g = math.gcd(group, 2)
    relay = 1
    chunks = q_cols // (g * HEAD)
    all_rows = rows * n_ctx
    dma = pltpu.SemaphoreType.DMA
    any_spec = pl.BlockSpec(memory_space=pl.ANY)
    return pl.pallas_call(
        functools.partial(kernel, n_sec, n_ctx, n_tp, g),
        out_shape=pltpu.VMEM((1, rows // n_tp, q_cols * n_tp), jnp.bfloat16),
        in_specs=[any_spec] * 4,
        out_specs=any_spec,
        scratch_shapes=[
            pltpu.VMEM((rows, q_cols - group * HEAD), jnp.bfloat16),
            pltpu.VMEM((rows, group * HEAD), jnp.bfloat16),
            pltpu.VMEM((2, rows, kv_cols), jnp.bfloat16),
            pltpu.VMEM((kv_heads, 2, all_rows, HEAD), jnp.bfloat16),
            pltpu.VMEM((chunks, rows, g * HEAD), jnp.bfloat16),
            pltpu.VMEM((relay, rows // n_tp, g * HEAD), jnp.bfloat16),
            pltpu.VMEM((rows, all_rows), jnp.float32),
            pltpu.SMEM(span_order.shape, jnp.int32),
            *[dma] * 4,
            dma((kv_heads,)),
            dma((2,)),
            *[dma] * 2,
            *[pltpu.SemaphoreType.REGULAR] * 2,
        ],
        compiler_params=pltpu.CompilerParams(collective_id=0, has_side_effects=True),
    )(queries, keys, values, span_order)


def solution(mesh):
    sizes = [mesh.shape[axis] for axis in ("section", "ctx", "tp")]
    placed = P("section", "ctx", "tp")
    return jax.shard_map(
        functools.partial(shards, *sizes),
        mesh=mesh,
        in_specs=(placed, placed, placed, P()),
        out_specs=P("section", ("ctx", "tp"), None),
        check_vma=False,
    )
```

```python
import functools
import math

import jax
import jax.numpy as jnp
from jax import lax
from jax.experimental import pallas as pl
from jax.experimental.pallas import tpu as pltpu
from jax.sharding import PartitionSpec as P

HEAD = 128
MESH = pl.DeviceIdType.MESH
NEG = -1e30
EARLY = 1


def lanes(start, size):
    return pl.ds(pl.multiple_of(start, HEAD), size)


def kernel(
    n_sec, n_ctx, n_tp, heads_per_chunk,
    q_hbm, k_hbm, v_hbm, order_hbm, out_hbm,
    q_buf, q_in, kv_own, kv_all, o_buf, relayed, bias, order,
    q_sem, own_sem, order_sem, sends, kv_recv, z_recv, o_recv, r_recv, pair_in, next_in,
):
    sec, ctx, tp = lax.axis_index("section"), lax.axis_index("ctx"), lax.axis_index("tp")
    rows, q_cols = q_hbm.shape[1], q_hbm.shape[2]
    kv_heads = k_hbm.shape[2] // HEAD
    group = q_cols // k_hbm.shape[2]
    g = heads_per_chunk
    chunk_cols = g * HEAD
    chunks = q_cols // chunk_cols
    per_kv = group // g
    out_rows = rows // n_tp
    keys = rows * n_ctx
    span = rows // 2
    local = kv_heads - 1
    group_cols = group * HEAD
    moved_cols = pl.ds(local * group_cols, group_cols)
    nxt, prv = lax.rem(sec + 1, n_sec), lax.rem(sec + n_sec - 1, n_sec)

    def there(s, c, t):
        return dict(device_id=(s, c, t), device_id_type=MESH)

    early = lax.rem(ctx, 2) == EARLY
    partner = ctx + 1 - 2 * lax.rem(ctx, 2)
    barrier = pltpu.get_barrier_semaphore()
    pl.semaphore_signal(barrier, inc=1, **there(prv, ctx, tp))
    for d in range(1, n_ctx):
        peer = lax.rem(ctx + d, n_ctx)

        @pl.when(lax.rem(peer, 2) != EARLY)
        def _():
            pl.semaphore_signal(barrier, inc=1, **there(sec, peer, tp))

    @pl.when(jnp.logical_not(early))
    def _():
        for d in range(1, n_tp):
            pl.semaphore_signal(barrier, inc=1, **there(sec, ctx, lax.rem(tp + d, n_tp)))

    def arrived(ref, sem):
        pltpu.make_async_copy(ref, ref, sem).wait()

    def left(ref, sem):
        pltpu.make_async_remote_copy(
            src_ref=ref, dst_ref=ref, send_sem=sem, recv_sem=sem, **there(nxt, ctx, tp)
        ).wait_send()

    kept_cols = pl.ds(0, local * group_cols)
    order_copy = pltpu.make_async_copy(order_hbm, order, order_sem)

    def load():
        for i, src in enumerate((k_hbm, v_hbm)):
            pltpu.make_async_copy(src.at[0], kv_own.at[i], own_sem).start()
        order_copy.start()
        pltpu.make_async_copy(q_hbm.at[0, :, kept_cols], q_buf, q_sem).start()

    pl.when(jnp.logical_not(early))(load)

    def greet_tp():
        for d in range(1, n_tp):
            pl.semaphore_signal(next_in, inc=1, **there(sec, ctx, lax.rem(tp + d, n_tp)))

    pl.semaphore_wait(barrier, jnp.where(early, 1, n_ctx + n_tp - 1))

    @pl.when(jnp.logical_not(early))
    def _():
        pl.semaphore_signal(pair_in, inc=1, **there(sec, partner, tp))
        greet_tp()

    others = pl.ds(0, keys - rows)
    mine = pl.ds(pl.multiple_of(ctx * rows, rows), rows)

    def kv_copy(i, h, d):
        dst = kv_all.at[h, i, mine, :]
        return pltpu.make_async_remote_copy(
            src_ref=kv_own.at[i, :, pl.ds(h * HEAD, HEAD)] if h < local else dst,
            dst_ref=dst,
            send_sem=sends,
            recv_sem=kv_recv.at[h],
            **there(sec, lax.rem(ctx + d, n_ctx), tp),
        )

    def section_copy(src, dst, recv_sem):
        return pltpu.make_async_remote_copy(
            src_ref=src, dst_ref=dst, send_sem=sends, recv_sem=recv_sem, **there(nxt, ctx, tp)
        )

    section_copy(q_hbm.at[0, :, moved_cols], q_in, z_recv.at[1]).start()
    for i, src in enumerate((k_hbm, v_hbm)):
        section_copy(
            src.at[0, :, pl.ds(local * HEAD, HEAD)], kv_all.at[local, i, mine, :], z_recv.at[0]
        ).start()
    pl.when(early)(load)
    arrived(kv_own, own_sem)

    @pl.when(early)
    def _():
        pl.semaphore_wait(pair_in, 1)

    for h in range(local):
        for i in range(2):
            for d in range(1, n_ctx):
                kv_copy(i, h, d).start()
    for h in range(local):
        for i in range(2):
            kv_all[h, i, mine, :] = kv_own[i, :, h * HEAD : (h + 1) * HEAD]

    order_copy.wait()
    row = lax.broadcasted_iota(jnp.int32, (rows, 1), 0)
    row_pos = jnp.where(row < span, order[2 * ctx] * span, order[2 * ctx + 1] * span - span) + row
    lane = lax.broadcasted_iota(jnp.int32, (1, keys), 1)
    key_pos = lane
    for j in range(keys // span):
        key_pos = jnp.where(
            (lane >= j * span) & (lane < (j + 1) * span), lane + (order[j] - j) * span, key_pos
        )
    bias[...] = jnp.where(key_pos <= row_pos, jnp.float32(0.0), jnp.float32(NEG))

    sent = local * per_kv
    late = 3
    scale = math.log2(math.e) / math.sqrt(HEAD)

    def out_copy(c, t):
        return pltpu.make_async_remote_copy(
            src_ref=o_buf.at[c, pl.ds(pl.multiple_of(t * out_rows, out_rows), out_rows), :],
            dst_ref=out_hbm.at[0, :, lanes(tp * q_cols + c * chunk_cols, chunk_cols)],
            send_sem=sends,
            recv_sem=o_recv,
            **there(nxt, ctx, t),
        )

    n_relay = relayed.shape[0]
    relays = n_tp > 1 and n_ctx % 4 == 0
    gives = jnp.logical_and(lax.rem(ctx, 4) == 1, tp == 0)
    takes = jnp.logical_and(lax.rem(ctx, 4) == 2, tp == 1)

    def give(c):
        pltpu.make_async_remote_copy(
            src_ref=o_buf.at[c, pl.ds(out_rows, out_rows), :],
            dst_ref=relayed.at[c],
            send_sem=sends,
            recv_sem=r_recv,
            **there(sec, lax.rem(ctx + 1, n_ctx), 1),
        ).start()

    def pass_on(c):
        return pltpu.make_async_remote_copy(
            src_ref=relayed.at[c],
            dst_ref=out_hbm.at[0, :, pl.ds(c * chunk_cols, chunk_cols)],
            send_sem=sends,
            recv_sem=o_recv,
            **there(nxt, lax.rem(ctx + n_ctx - 1, n_ctx), 1),
        )

    def send_late(c):
        if relays:
            @pl.when(jnp.logical_not(jnp.logical_and(gives, c < n_relay)))
            def _():
                out_copy(c, 1).start()

        for t in range(2 if relays else 1, n_tp):
            out_copy(c, t).start()

    def moved_out(c, d):
        t = lax.rem(tp + d, n_tp)
        src = o_buf.at[c, pl.ds(pl.multiple_of(t * out_rows, out_rows), out_rows), :]
        dst = out_hbm.at[0, :, lanes(tp * q_cols + c * chunk_cols, chunk_cols)]
        if d == 0:
            return pltpu.make_async_copy(src, dst, o_recv)
        return pltpu.make_async_remote_copy(
            src_ref=src,
            dst_ref=dst,
            send_sem=sends,
            recv_sem=o_recv,
            **there(sec, ctx, t),
        )

    for h in range(kv_heads):
        if h == 0:
            @pl.when(early)
            def _():
                pl.semaphore_wait(pair_in, 1)
                greet_tp()

            pl.semaphore_wait(next_in, n_tp - 1)

            @pl.when(jnp.logical_not(early))
            def _():
                pl.semaphore_signal(pair_in, inc=1, **there(sec, partner, tp))

            arrived(q_buf, q_sem)
        arrived(kv_all.at[h, :, others, :], kv_recv.at[h])

        def chunk(i, _, h=h):
            c = h * per_kv + i
            q_ref, first = (q_buf, c * g) if h < local else (q_in, i * g)
            q = jnp.concatenate(
                [q_ref[:, lanes((first + j) * HEAD, HEAD)] for j in range(g)], axis=0
            )
            s = lax.dot_general(
                q, kv_all[h, 0], (((1,), (1,)), ((), ())), preferred_element_type=jnp.float32
            )
            s = s.reshape(g, rows, keys) * scale + bias[...][None]
            m = jnp.max(s, axis=-1, keepdims=True)
            p = jnp.exp2(s - m)
            total = jnp.sum(p, axis=-1, keepdims=True)
            o = jnp.dot(
                p.astype(jnp.bfloat16).reshape(g * rows, keys),
                kv_all[h, 1],
                preferred_element_type=jnp.float32,
            ).reshape(g, rows, HEAD)
            o = (o / total).astype(jnp.bfloat16)
            for j in range(g):
                o_buf[c, :, j * HEAD : (j + 1) * HEAD] = o[j]
            if h < local:
                if relays:
                    @pl.when(jnp.logical_and(gives, c < n_relay))
                    def _():
                        give(c)

                out_copy(c, 0).start()

                @pl.when(c >= late)
                def _():
                    send_late(c - late)
            else:
                for d in range(n_tp):
                    moved_out(c, d).start()
            return 0

        lax.fori_loop(0, per_kv, chunk, 0)
        if h == local - 1:
            if relays:
                @pl.when(takes)
                def _():
                    arrived(relayed, r_recv)
                    for c in range(n_relay):
                        pass_on(c).start()

            for c in range(max(sent - late, 0), sent):
                send_late(c)
        if h == min(1, local - 1):
            arrived(kv_all.at[local, :, mine, :], z_recv.at[0])
            for i in range(2):
                for d in range(1, n_ctx):
                    kv_copy(i, local, d).start()
        if h == local - 1:
            arrived(q_in, z_recv.at[1])

    kept = chunks - sent
    left(q_in, sends)
    left(kv_all.at[0, :, mine, :], sends)
    left(kv_all.at[:, :, others, :], sends)
    if n_tp > 1:
        left(out_hbm.at[0, :, pl.ds(0, (n_tp - 1) * kept * chunk_cols)], sends)
    left(q_buf, sends)
    if relays:
        @pl.when(takes)
        def _():
            left(relayed, sends)

    arrived(out_hbm.at[0], o_recv)


def shards(n_sec, n_ctx, n_tp, queries, keys, values, span_order):
    rows, q_cols, kv_cols = queries.shape[1], queries.shape[2], keys.shape[2]
    kv_heads = kv_cols // HEAD
    group = q_cols // kv_cols
    g = math.gcd(group, 2)
    relay = 1
    chunks = q_cols // (g * HEAD)
    all_rows = rows * n_ctx
    dma = pltpu.SemaphoreType.DMA
    any_spec = pl.BlockSpec(memory_space=pl.ANY)
    return pl.pallas_call(
        functools.partial(kernel, n_sec, n_ctx, n_tp, g),
        out_shape=pltpu.VMEM((1, rows // n_tp, q_cols * n_tp), jnp.bfloat16),
        in_specs=[any_spec] * 4,
        out_specs=any_spec,
        scratch_shapes=[
            pltpu.VMEM((rows, q_cols - group * HEAD), jnp.bfloat16),
            pltpu.VMEM((rows, group * HEAD), jnp.bfloat16),
            pltpu.VMEM((2, rows, kv_cols), jnp.bfloat16),
            pltpu.VMEM((kv_heads, 2, all_rows, HEAD), jnp.bfloat16),
            pltpu.VMEM((chunks, rows, g * HEAD), jnp.bfloat16),
            pltpu.VMEM((relay, rows // n_tp, g * HEAD), jnp.bfloat16),
            pltpu.VMEM((rows, all_rows), jnp.float32),
            pltpu.SMEM(span_order.shape, jnp.int32),
            *[dma] * 4,
            dma((kv_heads,)),
            dma((2,)),
            *[dma] * 2,
            *[pltpu.SemaphoreType.REGULAR] * 2,
        ],
        compiler_params=pltpu.CompilerParams(collective_id=0, has_side_effects=True),
    )(queries, keys, values, span_order)


def solution(mesh):
    sizes = [mesh.shape[axis] for axis in ("section", "ctx", "tp")]
    placed = P("section", "ctx", "tp")
    return jax.shard_map(
        functools.partial(shards, *sizes),
        mesh=mesh,
        in_specs=(placed, placed, placed, P()),
        out_specs=P("section", ("ctx", "tp"), None),
        check_vma=False,
    )
```
